32 devices in a mesh: node: 4 (over y, x), intra: 8 (over z, core).
Axes of the slice: x: 2, y: 2, z: 4, core: 2. Of those that a mesh axis runs over, the one named last changes fastest.
Arguments:
- gradients: bfloat16 [4, 8, 3072, 512], P('node', 'intra'), as said below
- sign_table: int32 [64, 512], replicated, may hold values from -1 to 1, as said below
- loss_scale: float32 [1], replicated, may hold values from 256 to 65536
- step_count: int32 [1], replicated, may hold values from 1 to 8
- weights: float32 [3072, 512], P('intra', 'node'), may hold values from -6 to 6
- first_moment: float32 [3072, 512], P('intra', 'node'), may hold values from -3 to 3
- second_moment: float32 [3072, 512], P('intra', 'node'), may hold values from 0.01 to 0.1
Outputs:
- new_weights: float32 [3072, 512], P('intra', 'node')
- new_first: float32 [3072, 512], P('intra', 'node')
- new_second: float32 [3072, 512], P('intra', 'node')
The draws below stay inside these ranges and needn't reach their ends.
Inputs may be any that keep to these rules, and one draw needn't show every extreme that they name: `gradients`: each replica's gradient is multiplied by loss_scale. `sign_table`: every entry is -1 or 1.
All inputs are finite; a program needn't handle non-finite values.
Results may differ from the reference program's by a relative error of at most 0.0003.
Values sent between devices are 32-bit elements; how exact they have to be, the bound alone decides.
A program may use at most 128 MiB of HBM per device.

```python
import math
import jax
import jax.numpy as jnp
from jax import lax

BLOCK = 128
SIGN_ROWS = 64
GRAD_ROWS = 3072
GRAD_COLS = 512
N_NODE = 4
N_INTRA = 8


def shared_scale(key):
    fraction = jax.random.uniform(jax.random.fold_in(key, 11), (), jnp.float32)
    return jnp.exp(jnp.log(256.0) + fraction * (jnp.log(65536.0) - jnp.log(256.0)))


def draw_loss_scale(key, part):
    return shared_scale(key).reshape(1).astype(jnp.float32)


def draw_gradients(key, part):
    replicas = N_NODE * N_INTRA
    ranking = jnp.arange(replicas, dtype=jnp.float32) / (replicas - 1)
    jitter = jax.random.uniform(jax.random.fold_in(key, 1), (replicas,), jnp.float32, 0.8, 1.25)
    device_scale = jnp.power(3.0, ranking) * jitter
    noise = jax.random.truncated_normal(jax.random.fold_in(key, 2), -6.0, 6.0, (replicas, GRAD_ROWS, GRAD_COLS), jnp.float32)
    values = noise * device_scale[:, None, None] * shared_scale(key)
    return values.reshape(N_NODE, N_INTRA, GRAD_ROWS, GRAD_COLS).astype(jnp.bfloat16)


def draw_sign_table(key, part):
    return 2 * jax.random.randint(jax.random.fold_in(key, 21), (SIGN_ROWS, GRAD_COLS), 0, 2, jnp.int32) - 1


def level_of(rng, dims, cuts, low, high):
    def one(position, blocks):
        steps = jax.random.uniform(jax.random.fold_in(jax.random.fold_in(rng, 6), position), (blocks,), jnp.float32, low / len(cuts), high / len(cuts))
        return jnp.repeat(jnp.exp(steps), dims[position] // blocks).reshape((-1,) + (1,) * (len(dims) - position - 1))

    loudness = one(*cuts[0])
    for cut in cuts[1:]:
        loudness = loudness * one(*cut)
    return loudness


def bell_draw(key, shape, scale, most, cuts=(), held_as=jnp.bfloat16):
    level = level_of(key, shape, cuts, -0.22, 0.18) if cuts else 1.0
    array = jax.random.normal(key, shape, jnp.float32) * scale * level
    return jnp.minimum(jnp.maximum(array, -most), most).astype(held_as)


def setup_inputs(seed: int = 0) -> dict:
    arg_keys = jax.random.split(jax.random.key(seed), 8)
    return {
        "gradients": draw_gradients(jax.random.fold_in(arg_keys[7], 71), 0),
        "sign_table": draw_sign_table(jax.random.fold_in(arg_keys[7], 71), 0),
        "loss_scale": draw_loss_scale(jax.random.fold_in(arg_keys[7], 71), 0),
        "step_count": jax.random.randint(arg_keys[3], (1,), 1, 9).astype(jnp.int32),
        "weights": bell_draw(arg_keys[4], (GRAD_ROWS, GRAD_COLS), 1.0, 6.0, ((0, 8), (1, 4)), jnp.float32),
        "first_moment": bell_draw(arg_keys[5], (GRAD_ROWS, GRAD_COLS), 0.2, 3.0, ((0, 8), (1, 4)), jnp.float32),
        "second_moment": jnp.clip(jnp.exp(math.log(0.1) - 2.3025851 * jax.random.uniform(arg_keys[6], (GRAD_ROWS, GRAD_COLS), jnp.float32) ** level_of(arg_keys[6], (GRAD_ROWS, GRAD_COLS), ((0, 8), (1, 4)), -0.2, 0.2)), 0.01, 0.1),
    }


def hadamard(order):
    index = jnp.arange(order, dtype=jnp.int32)
    common = index[:, None] & index[None, :]
    parity = jnp.zeros((order, order), jnp.int32)
    for bit_index in range(order.bit_length() - 1):
        parity = parity ^ common >> bit_index & 1
    return 1 - 2 * parity

def reference(gradients, sign_table, loss_scale, step_count, weights, first_moment, second_moment):
    table_int = hadamard(BLOCK)
    table_half = table_int.astype(jnp.bfloat16)
    table_full = table_int.astype(jnp.float32)
    inverse_root = 1.0 / math.sqrt(BLOCK)
    sign_tile = jnp.tile(sign_table, (GRAD_ROWS // SIGN_ROWS, 1))
    sign_half = sign_tile.astype(jnp.bfloat16)
    replicas = gradients.reshape(N_NODE * N_INTRA, GRAD_ROWS, GRAD_COLS)

    def rotate(replica):
        signed = (replica * sign_half).reshape(-1, BLOCK)
        spun = jnp.dot(signed, table_half, preferred_element_type=jnp.float32) * inverse_root
        return spun.reshape(GRAD_ROWS, GRAD_COLS)
    maxima = lax.map(lambda replica: jnp.max(jnp.abs(rotate(replica))), replicas)
    top_value = jnp.max(maxima)
    level_scale = 127.0 / top_value

    def accumulate(carry, replica):
        levels = jnp.floor(rotate(replica) * level_scale + 0.5)
        return (carry + levels, None)
    summed, _ = lax.scan(accumulate, jnp.zeros((GRAD_ROWS, GRAD_COLS), jnp.float32), replicas)
    factor = top_value / (127.0 * (N_NODE * N_INTRA) * loss_scale[0])
    scaled = (summed * factor).reshape(-1, BLOCK)
    back = jnp.dot(scaled, table_full, precision=lax.Precision.HIGHEST) * inverse_root
    grad = back.reshape(GRAD_ROWS, GRAD_COLS) * sign_tile.astype(jnp.float32)
    new_first = 0.9 * first_moment + 0.1 * grad
    new_second = 0.95 * second_moment + 0.05 * grad * grad
    steps_float = step_count[0].astype(jnp.float32)
    first_hat = new_first / (1.0 - jnp.power(jnp.float32(0.9), steps_float))
    second_hat = new_second / (1.0 - jnp.power(jnp.float32(0.95), steps_float))
    update = first_hat / (jnp.sqrt(second_hat) + 1e-08) + 0.1 * weights
    new_weights = weights - 0.2 * update
    return (new_weights, new_first, new_second)
```

```python
import functools
import math

import jax
import jax.numpy as jnp
from jax import lax
from jax.experimental import pallas as pl
from jax.experimental.pallas import tpu as pltpu
from jax.sharding import PartitionSpec as P

BLOCK = 128
SIGN_ROWS = 64
CORES = 2
SLOTS = 4
ROOT = 1.0 / math.sqrt(BLOCK)
MESH = pl.DeviceIdType.MESH


def hadamard(order):
    index = jnp.arange(order, dtype=jnp.int32)
    common = index[:, None] & index[None, :]
    parity = jnp.zeros((order, order), jnp.int32)
    for bit_index in range(order.bit_length() - 1):
        parity = parity ^ common >> bit_index & 1
    return 1 - 2 * parity


def reduce_kernel(
    n_node, n_intra, grad_ref, sign_ref, table_ref, sum_ref, top_ref,
    stage, lev, pair, first, second, up, down, peak, near, far,
    load_sem, pair_send, pair_recv, first_send, first_recv, second_send, second_recv,
    up_send, up_recv, down_send, down_recv, near_send, near_recv, far_send, far_recv,
):
    lo_count = 2
    n_z = n_intra // CORES
    owned = lev.shape[4] * 2
    node, intra = lax.axis_index("node"), lax.axis_index("intra")
    z, core = intra // CORES, intra % CORES
    hi, lo = node // lo_count, node % lo_count
    group = n_node * CORES
    me = node * CORES + core

    def at(node_index, z_index, core_index):
        return (node_index, z_index * CORES + core_index)

    def load(i):
        slot = lax.rem(i, SLOTS)
        return pltpu.make_async_copy(
            grad_ref.at[pl.ds(i * owned, owned)], stage.at[slot], load_sem.at[slot]
        )

    for i in range(min(SLOTS, n_intra)):
        load(i).start()

    barrier = pltpu.get_barrier_semaphore()
    for step in range(1, group):
        other = lax.rem(me + step, group)
        pl.semaphore_signal(
            barrier, inc=1, device_id=at(other // CORES, z, other % CORES), device_id_type=MESH
        )
    for step in range(1, n_z):
        pl.semaphore_signal(
            barrier, inc=1, device_id=at(node, lax.rem(z + step, n_z), core), device_id_type=MESH
        )

    table = table_ref[...]
    signs = sign_ref[...].astype(jnp.float32).astype(jnp.bfloat16)
    half = owned // 2

    def rotate(i, most):
        load(i).wait()
        block = stage[lax.rem(i, SLOTS)]
        for j in range(n_node):
            cols = slice(j * BLOCK, (j + 1) * BLOCK)
            part = block[:, cols].reshape(owned // SIGN_ROWS, SIGN_ROWS, BLOCK)
            signed = (part * signs[:, cols][None]).reshape(owned, BLOCK)
            spun = jnp.dot(signed, table, preferred_element_type=jnp.float32) * ROOT
            for h in range(2):
                lev[i, j // lo_count, j % lo_count, h] = spun[h * half : (h + 1) * half]
            most = jnp.maximum(most, jnp.max(jnp.abs(spun).reshape(owned // 8, 8, BLOCK), axis=0))

        @pl.when(i + SLOTS < n_intra)
        def _():
            load(i + SLOTS).start()

        return most

    most = lax.fori_loop(0, n_intra, rotate, jnp.zeros((8, BLOCK), jnp.float32))

    pl.semaphore_wait(barrier, group - 1 + n_z - 1)

    def near_copy(target, slot):
        return pltpu.make_async_remote_copy(
            src_ref=peak.at[0], dst_ref=near.at[slot], send_sem=near_send.at[target],
            recv_sem=near_recv.at[slot], device_id=at(target // CORES, z, target % CORES),
            device_id_type=MESH,
        )

    def far_copy(target, slot):
        return pltpu.make_async_remote_copy(
            src_ref=peak.at[1], dst_ref=far.at[slot], send_sem=far_send.at[target],
            recv_sem=far_recv.at[slot], device_id=at(node, target, core), device_id_type=MESH,
        )

    peak[0] = most
    for step in range(1, group):
        near_copy(lax.rem(me + step, group), me).start()
    for step in range(1, group):
        other = lax.rem(me + step, group)
        near_copy(other, other).wait_recv()
        most = jnp.maximum(most, near[other])
    peak[1] = most
    for step in range(1, n_z):
        far_copy(lax.rem(z + step, n_z), z).start()
    for step in range(1, n_z):
        other = lax.rem(z + step, n_z)
        far_copy(other, other).wait_recv()
        most = jnp.maximum(most, far[other])
    top_value = jnp.max(jnp.max(most, axis=0, keepdims=True), axis=1, keepdims=True)
    top_ref[...] = jnp.broadcast_to(top_value, (8, BLOCK))
    level_scale = 127.0 / top_value

    def piece(k):
        last = n_z - 1
        lower = jnp.where(k < last - z, last - k, k - (last - z))
        upper = jnp.where(k < z, k, last - (k - z))
        return jnp.where(z < n_z // 2, lower, upper)

    def pair_copy(p):
        return pltpu.make_async_remote_copy(
            src_ref=lev.at[p * CORES + 1 - core], dst_ref=pair.at[p], send_sem=pair_send.at[p],
            recv_sem=pair_recv.at[p], device_id=at(node, z, 1 - core), device_id_type=MESH,
        )

    lo_peer = hi * lo_count + 1 - lo
    hi_peer = (1 - hi) * lo_count + lo

    def first_copies(p):
        i = p * CORES + core
        return [
            pltpu.make_async_remote_copy(
                src_ref=src, dst_ref=first.at[p, h], send_sem=first_send.at[h, p],
                recv_sem=first_recv.at[h, p], device_id=at(peer, z, core), device_id_type=MESH,
            )
            for h, src, peer in (
                (0, lev.at[i, :, 1 - lo, 0], lo_peer),
                (1, lev.at[i, 1 - hi, :, 1], hi_peer),
            )
        ]

    def second_copies(p):
        i = p * CORES + core
        return [
            pltpu.make_async_remote_copy(
                src_ref=src, dst_ref=second.at[p, h], send_sem=second_send.at[h, p],
                recv_sem=second_recv.at[h, p], device_id=at(peer, z, core), device_id_type=MESH,
            )
            for h, src, peer in (
                (0, lev.at[i, 1 - hi, lo, 0], hi_peer),
                (1, lev.at[i, hi, 1 - lo, 1], lo_peer),
            )
        ]

    def up_copy(p):
        return pltpu.make_async_remote_copy(
            src_ref=lev.at[p * CORES + core, hi, lo], dst_ref=up.at[p], send_sem=up_send.at[p],
            recv_sem=up_recv.at[p], device_id=at(node, lax.rem(z + 1, n_z), core),
            device_id_type=MESH,
        )

    def down_copy(p):
        return pltpu.make_async_remote_copy(
            src_ref=lev.at[p * CORES + core, hi, lo], dst_ref=down.at[p], send_sem=down_send.at[p],
            recv_sem=down_recv.at[p], device_id=at(node, lax.rem(z + n_z - 1, n_z), core),
            device_id_type=MESH,
        )

    def pipeline(t, carry):
        @pl.when(t < n_z)
        def _():
            p = piece(t)
            for c in range(CORES):
                i = p * CORES + lax.rem(core + 1 + c, CORES)
                for j in range(n_node):
                    for h in range(2):
                        spot = (i, j // lo_count, j % lo_count, h)
                        lev[spot] = jnp.floor(lev[spot] * level_scale + 0.5)
                if c == 0:
                    pair_copy(p).start()

        @pl.when((t >= 1) & (t < n_z + 1))
        def _():
            p = piece(t - 1)
            i = p * CORES + core
            pair_copy(p).wait_recv()
            for j in range(n_node):
                for h in range(2):
                    spot = (j // lo_count, j % lo_count, h)
                    lev[(i,) + spot] = lev[(i,) + spot] + pair[(p,) + spot]
            for copy in first_copies(p):
                copy.start()

        @pl.when((t >= 2) & (t < n_z + 2))
        def _():
            p = piece(t - 2)
            i = p * CORES + core
            for copy in first_copies(p):
                copy.wait_recv()
            for j in range(2):
                lev[i, j, lo, 0] = lev[i, j, lo, 0] + first[p, 0, j]
                lev[i, hi, j, 1] = lev[i, hi, j, 1] + first[p, 1, j]
            for copy in second_copies(p):
                copy.start()

        @pl.when(t >= 3)
        def _():
            p = piece(t - 3)
            i = p * CORES + core
            for copy in second_copies(p):
                copy.wait_recv()
            for h in range(2):
                lev[i, hi, lo, h] = lev[i, hi, lo, h] + second[p, h]

            @pl.when((p >= z) & (z > 0))
            def _():
                up_copy(p).wait_recv()
                lev[i, hi, lo] = lev[i, hi, lo] + up[p]

            @pl.when((p <= z) & (z < n_z - 1))
            def _():
                down_copy(p).wait_recv()
                lev[i, hi, lo] = lev[i, hi, lo] + down[p]

            @pl.when(p > z)
            def _():
                up_copy(p).start()

            @pl.when(p < z)
            def _():
                down_copy(p).start()

        return carry

    lax.fori_loop(0, n_z + 3, pipeline, 0)

    for h in range(2):
        sum_ref[h * half : (h + 1) * half, :] = lev[intra, hi, lo, h]

    for step in range(1, group):
        near_copy(lax.rem(me + step, group), me).wait_send()
    for step in range(1, n_z):
        far_copy(lax.rem(z + step, n_z), z).wait_send()

    def finish(p, carry):
        pair_copy(p).wait_send()
        for copy in first_copies(p) + second_copies(p):
            copy.wait_send()

        @pl.when(p > z)
        def _():
            up_copy(p).wait_send()

        @pl.when(p < z)
        def _():
            down_copy(p).wait_send()

        return carry

    lax.fori_loop(0, n_z, finish, 0)


def adam_kernel(
    replicas, sum_ref, top_ref, sign_ref, table_ref, scale_ref, step_ref,
    weight_ref, first_ref, second_ref, new_weight_ref, new_first_ref, new_second_ref,
):
    owned = sum_ref.shape[0]
    table = table_ref[...]
    summed = sum_ref[...]
    high = jnp.floor(summed * (1.0 / 64.0))
    low = summed - high * 64.0
    back = jnp.dot(high.astype(jnp.bfloat16), table, preferred_element_type=jnp.float32) * 64.0
    back = back + jnp.dot(low.astype(jnp.bfloat16), table, preferred_element_type=jnp.float32)
    ones = jnp.ones((1, BLOCK), jnp.float32)
    factor = top_ref[0:1, :] / (ones * (127.0 * replicas * scale_ref[0]))
    signs = sign_ref[...].astype(jnp.float32) * (factor * ROOT)
    grad = (back.reshape(owned // SIGN_ROWS, SIGN_ROWS, BLOCK) * signs[None]).reshape(owned, BLOCK)
    steps = ones * step_ref[0].astype(jnp.float32)
    first_unbias = 1.0 / (1.0 - jnp.exp(steps * math.log(0.9)))
    second_unbias = 1.0 / (1.0 - jnp.exp(steps * math.log(0.95)))
    new_first = 0.9 * first_ref[...] + 0.1 * grad
    new_second = 0.95 * second_ref[...] + 0.05 * grad * grad
    new_first_ref[...] = new_first
    new_second_ref[...] = new_second
    weights = weight_ref[...]
    update = (new_first * first_unbias) / (jnp.sqrt(new_second * second_unbias) + 1e-08)
    new_weight_ref[...] = weights - 0.2 * (update + 0.1 * weights)


def shards(gradients, sign_table, loss_scale, step_count, weights, first_moment, second_moment):
    n_node, n_intra = lax.axis_size("node"), lax.axis_size("intra")
    n_z = n_intra // CORES
    local = gradients.reshape(gradients.shape[2:])
    rows, columns = local.shape
    owned = weights.shape[0]
    half = owned // 2
    n_hi = n_node // 2
    table = hadamard(BLOCK).astype(jnp.bfloat16)
    vmem = pl.BlockSpec(memory_space=pltpu.VMEM)
    smem = pl.BlockSpec(memory_space=pltpu.SMEM)
    dma = pltpu.SemaphoreType.DMA
    group = n_node * CORES
    f32 = jnp.float32
    summed, top = pl.pallas_call(
        functools.partial(reduce_kernel, n_node, n_intra),
        out_shape=(
            jax.ShapeDtypeStruct((owned, BLOCK), f32),
            jax.ShapeDtypeStruct((8, BLOCK), f32),
        ),
        in_specs=[pl.BlockSpec(memory_space=pl.ANY), vmem, vmem],
        out_specs=(vmem, vmem),
        scratch_shapes=[
            pltpu.VMEM((SLOTS, owned, columns), jnp.bfloat16),
            pltpu.VMEM((n_intra, n_hi, 2, 2, half, BLOCK), f32),
            pltpu.VMEM((n_z, n_hi, 2, 2, half, BLOCK), f32),
            pltpu.VMEM((n_z, 2, 2, half, BLOCK), f32),
            pltpu.VMEM((n_z, 2, half, BLOCK), f32),
            pltpu.VMEM((n_z, 2, half, BLOCK), f32),
            pltpu.VMEM((n_z, 2, half, BLOCK), f32),
            pltpu.VMEM((2, 8, BLOCK), f32),
            pltpu.VMEM((group, 8, BLOCK), f32),
            pltpu.VMEM((n_z, 8, BLOCK), f32),
            dma((SLOTS,)),
            dma((n_z,)), dma((n_z,)),
            dma((2, n_z)), dma((2, n_z)),
            dma((2, n_z)), dma((2, n_z)),
            dma((n_z,)), dma((n_z,)),
            dma((n_z,)), dma((n_z,)),
            dma((group,)), dma((group,)),
            dma((n_z,)), dma((n_z,)),
        ],
        compiler_params=pltpu.CompilerParams(
            collective_id=0, has_side_effects=True, vmem_limit_bytes=60 * 1024 * 1024
        ),
    )(local, sign_table, table)
    own_signs = lax.dynamic_slice_in_dim(sign_table, lax.axis_index("node") * BLOCK, BLOCK, 1)
    shape = jax.ShapeDtypeStruct((owned, BLOCK), f32)
    return pl.pallas_call(
        functools.partial(adam_kernel, float(n_node * n_intra)),
        out_shape=(shape, shape, shape),
        in_specs=[vmem, vmem, vmem, vmem, smem, smem, vmem, vmem, vmem],
        out_specs=(vmem, vmem, vmem),
    )(summed, top, own_signs, table, loss_scale, step_count, weights, first_moment, second_moment)


def solution(mesh):
    own = P("intra", "node")
    return jax.shard_map(
        shards,
        mesh=mesh,
        in_specs=(P("node", "intra", None, None), P(), P(), P(), own, own, own),
        out_specs=(own, own, own),
        check_vma=False,
    )
```

```python
import functools
import math

import jax
import jax.numpy as jnp
from jax import lax
from jax.experimental import pallas as pl
from jax.experimental.pallas import tpu as pltpu
from jax.sharding import PartitionSpec as P

BLOCK = 128
SIGN_ROWS = 64
CORES = 2
SLOTS = 4
ROOT = 1.0 / math.sqrt(BLOCK)
MESH = pl.DeviceIdType.MESH


def hadamard_table():
    common = lax.broadcasted_iota(jnp.int32, (BLOCK, BLOCK), 0) & lax.broadcasted_iota(
        jnp.int32, (BLOCK, BLOCK), 1
    )
    parity = common
    for bit_index in range(1, BLOCK.bit_length() - 1):
        parity = parity ^ (common >> bit_index)
    return (1 - 2 * (parity & 1)).astype(jnp.float32).astype(jnp.bfloat16)


def reduce_kernel(
    n_node, n_intra, grad_ref, sign_ref, sum_ref, top_ref,
    stage, lev, pair, raw, first, second, third, peak, near, far,
    load_sem, pair_send, pair_recv, raw_send, raw_recv, first_send, first_recv,
    second_send, second_recv, third_send, third_recv, near_send, near_recv, far_send, far_recv,
):
    lo_count = 2
    n_z = n_intra // CORES
    owned = lev.shape[4] * 2
    half = owned // 2
    node, intra = lax.axis_index("node"), lax.axis_index("intra")
    z, core = intra // CORES, intra % CORES
    hi, lo = node // lo_count, node % lo_count
    group = n_node * CORES
    me = node * CORES + core

    def at(node_index, z_index, core_index):
        return (node_index, z_index * CORES + core_index)

    def send(src, dst, send_sem, recv_sem, device):
        return pltpu.make_async_remote_copy(
            src_ref=src, dst_ref=dst, send_sem=send_sem, recv_sem=recv_sem,
            device_id=device, device_id_type=MESH,
        )

    def piece(k):
        last = n_z - 1
        lower = jnp.where(k < last - z, last - k, k - (last - z))
        upper = jnp.where(k < z, k, last - (k - z))
        return jnp.where(z < n_z // 2, lower, upper)

    early = min(2, n_z)

    def block_at(q):
        other = (q >= early) & (q < early + n_z)
        k = jnp.where(q < early, q, jnp.where(other, q - early, q - n_z))
        return piece(k) * CORES + jnp.where(other, 1 - core, core)

    def load(q):
        slot = lax.rem(q, SLOTS)
        return pltpu.make_async_copy(
            grad_ref.at[pl.ds(block_at(q) * owned, owned)], stage.at[slot], load_sem.at[slot]
        )

    for q in range(min(SLOTS, n_intra)):
        load(q).start()

    barrier = pltpu.get_barrier_semaphore()
    for step in range(1, group):
        other = lax.rem(me + step, group)
        pl.semaphore_signal(
            barrier, inc=1, device_id=at(other // CORES, z, other % CORES), device_id_type=MESH
        )
    for step in range(1, n_z):
        pl.semaphore_signal(
            barrier, inc=1, device_id=at(node, lax.rem(z + step, n_z), core), device_id_type=MESH
        )

    table = hadamard_table()
    signs = sign_ref[...].astype(jnp.float32).astype(jnp.bfloat16)

    def rotate(q, most):
        load(q).wait()
        i = block_at(q)
        block = stage[lax.rem(q, SLOTS)]
        for j in range(n_node):
            cols = slice(j * BLOCK, (j + 1) * BLOCK)
            part = block[:, cols].reshape(owned // SIGN_ROWS, SIGN_ROWS, BLOCK)
            signed = (part * signs[:, cols][None]).reshape(owned, BLOCK)
            spun = jnp.dot(signed, table, preferred_element_type=jnp.float32) * ROOT
            for h in range(2):
                lev[i, j // lo_count, j % lo_count, h] = spun[h * half : (h + 1) * half]
            most = jnp.maximum(most, jnp.max(jnp.abs(spun).reshape(owned // 8, 8, BLOCK), axis=0))

        @pl.when(q + SLOTS < n_intra)
        def _():
            load(q + SLOTS).start()

        return most

    lo_peer = hi * lo_count + 1 - lo
    hi_peer = (1 - hi) * lo_count + lo

    def pair_copy(p):
        return send(
            lev.at[p * CORES + 1 - core], pair.at[p], pair_send.at[p], pair_recv.at[p],
            at(node, z, 1 - core),
        )

    def raw_copies(flip):
        target = core if flip == 0 else 1 - core
        i = piece(0) * CORES + target
        return [
            send(
                src, raw.at[flip, h], raw_send.at[flip, h], raw_recv.at[flip, h],
                at(peer, z, target),
            )
            for h, src, peer in (
                (0, lev.at[i, :, 1 - lo, 0], lo_peer),
                (1, lev.at[i, 1 - hi, :, 1], hi_peer),
            )
        ]

    def first_copies(p):
        i = p * CORES + core
        return [
            send(src, first.at[p, h], first_send.at[h, p], first_recv.at[h, p], at(peer, z, core))
            for h, src, peer in (
                (0, lev.at[i, :, 1 - lo, 0], lo_peer),
                (1, lev.at[i, 1 - hi, :, 1], hi_peer),
            )
        ]

    def second_copies(p):
        i = p * CORES + core
        return [
            send(
                src, second.at[p, h], second_send.at[h, p], second_recv.at[h, p],
                at(peer, z, core),
            )
            for h, src, peer in (
                (0, lev.at[i, 1 - hi, lo, 0], hi_peer),
                (1, lev.at[i, hi, 1 - lo, 1], lo_peer),
            )
        ]

    def third_copy(p, slot):
        return send(
            lev.at[p * CORES + core, hi, lo], third.at[slot], third_send.at[p],
            third_recv.at[slot], at(node, p, core),
        )

    def near_copy(target, slot):
        return send(
            peak.at[0], near.at[slot], near_send.at[target], near_recv.at[slot],
            at(target // CORES, z, target % CORES),
        )

    def far_copy(target, slot):
        return send(
            peak.at[1], far.at[slot], far_send.at[target], far_recv.at[slot],
            at(node, target, core),
        )

    most = lax.fori_loop(0, early, rotate, jnp.zeros((8, BLOCK), jnp.float32))
    pl.semaphore_wait(barrier, group - 1 + n_z - 1)
    for copy in raw_copies(0):
        copy.start()

    def rotate_and_send(q, most):
        most = rotate(q, most)
        pair_copy(piece(q - early)).start()
        return most

    most = lax.fori_loop(early, early + n_z, rotate_and_send, most)
    most = lax.fori_loop(early + n_z, n_intra, rotate, most)

    peak[0] = most
    for step in range(1, group):
        near_copy(lax.rem(me + step, group), me).start()
    for copy in raw_copies(1):
        copy.start()
    for step in range(1, group):
        other = lax.rem(me + step, group)
        near_copy(other, other).wait_recv()
        most = jnp.maximum(most, near[other])
    peak[1] = most
    for step in range(1, n_z):
        far_copy(lax.rem(z + step, n_z), z).start()
    for step in range(1, n_z):
        other = lax.rem(z + step, n_z)
        far_copy(other, other).wait_recv()
        most = jnp.maximum(most, far[other])
    top_value = jnp.max(jnp.max(most, axis=0, keepdims=True), axis=1, keepdims=True)
    top_ref[...] = jnp.broadcast_to(top_value, (8, BLOCK))
    level_scale = 127.0 / top_value

    def level(value):
        return jnp.floor(value * level_scale + 0.5)

    def pipeline(t, carry):
        @pl.when(t < n_z)
        def _():
            p = piece(t)
            i = p * CORES + core
            pair_copy(p).wait_recv()
            for j in range(n_node):
                for h in range(2):
                    spot = (j // lo_count, j % lo_count, h)
                    lev[(i,) + spot] = level(lev[(i,) + spot]) + level(pair[(p,) + spot])
            for copy in first_copies(p):
                copy.start()

        @pl.when(t == 1)
        def _():
            p = piece(0)
            i = p * CORES + core
            pair_copy(p).wait_recv()
            for flip in range(2):
                for copy in raw_copies(flip):
                    copy.wait_recv()

            def kept(h, j, spot):
                lev[(i,) + spot] = (
                    level(lev[(i,) + spot]) + level(pair[(p,) + spot])
                    + level(raw[0, h, j]) + level(raw[1, h, j])
                )

            for j in range(2):
                kept(0, j, (j, lo, 0))
                kept(1, j, (hi, j, 1))
            for copy in second_copies(p):
                copy.start()

        @pl.when((t >= 2) & (t <= n_z))
        def _():
            p = piece(t - 1)
            i = p * CORES + core
            for copy in first_copies(p):
                copy.wait_recv()
            for j in range(2):
                lev[i, j, lo, 0] = lev[i, j, lo, 0] + first[p, 0, j]
                lev[i, hi, j, 1] = lev[i, hi, j, 1] + first[p, 1, j]
            for copy in second_copies(p):
                copy.start()

        @pl.when(t >= 2)
        def _():
            p = piece(t - 2)
            i = p * CORES + core
            for copy in second_copies(p):
                copy.wait_recv()
            for h in range(2):
                lev[i, hi, lo, h] = lev[i, hi, lo, h] + second[p, h]

            @pl.when(p != z)
            def _():
                third_copy(p, z).start()

        return carry

    lax.fori_loop(1, n_z + 2, pipeline, 0)

    total = lev[intra, hi, lo]
    for step in range(1, n_z):
        other = lax.rem(z + step, n_z)
        third_copy(other, other).wait_recv()
        total = total + third[other]
    for h in range(2):
        sum_ref[h * half : (h + 1) * half, :] = total[h]

    for step in range(1, group):
        near_copy(lax.rem(me + step, group), me).wait_send()
    for step in range(1, n_z):
        far_copy(lax.rem(z + step, n_z), z).wait_send()
    for flip in range(2):
        for copy in raw_copies(flip):
            copy.wait_send()

    def finish(k, carry):
        p = piece(k)
        pair_copy(p).wait_send()
        for copy in second_copies(p):
            copy.wait_send()

        @pl.when(k > 0)
        def _():
            for copy in first_copies(p):
                copy.wait_send()

        @pl.when(p != z)
        def _():
            third_copy(p, z).wait_send()

        return carry

    lax.fori_loop(0, n_z, finish, 0)


def adam_kernel(
    replicas, sum_ref, top_ref, sign_ref, scale_ref, step_ref,
    weight_ref, first_ref, second_ref, new_weight_ref, new_first_ref, new_second_ref,
):
    owned = sum_ref.shape[0]
    table = hadamard_table()
    column = pl.multiple_of(lax.axis_index("node") * BLOCK, BLOCK)
    summed = sum_ref[...]
    high = jnp.floor(summed * (1.0 / 64.0))
    low = summed - high * 64.0
    back = jnp.dot(high.astype(jnp.bfloat16), table, preferred_element_type=jnp.float32) * 64.0
    back = back + jnp.dot(low.astype(jnp.bfloat16), table, preferred_element_type=jnp.float32)
    ones = jnp.ones((1, BLOCK), jnp.float32)
    factor = top_ref[0:1, :] / (ones * (127.0 * replicas * scale_ref[0]))
    signs = sign_ref[:, pl.ds(column, BLOCK)].astype(jnp.float32) * (factor * ROOT)
    grad = (back.reshape(owned // SIGN_ROWS, SIGN_ROWS, BLOCK) * signs[None]).reshape(owned, BLOCK)
    steps = ones * step_ref[0].astype(jnp.float32)
    first_unbias = 1.0 / (1.0 - jnp.exp(steps * math.log(0.9)))
    second_unbias = 1.0 / (1.0 - jnp.exp(steps * math.log(0.95)))
    new_first = 0.9 * first_ref[...] + 0.1 * grad
    new_second = 0.95 * second_ref[...] + 0.05 * grad * grad
    new_first_ref[...] = new_first
    new_second_ref[...] = new_second
    weights = weight_ref[...]
    update = (new_first * first_unbias) / (jnp.sqrt(new_second * second_unbias) + 1e-08)
    new_weight_ref[...] = weights - 0.2 * (update + 0.1 * weights)


def shards(gradients, sign_table, loss_scale, step_count, weights, first_moment, second_moment):
    n_node, n_intra = lax.axis_size("node"), lax.axis_size("intra")
    n_z = n_intra // CORES
    local = gradients.reshape(gradients.shape[2:])
    rows, columns = local.shape
    owned = weights.shape[0]
    half = owned // 2
    n_hi = n_node // 2
    vmem = pl.BlockSpec(memory_space=pltpu.VMEM)
    smem = pl.BlockSpec(memory_space=pltpu.SMEM)
    dma = pltpu.SemaphoreType.DMA
    group = n_node * CORES
    f32 = jnp.float32
    summed, top = pl.pallas_call(
        functools.partial(reduce_kernel, n_node, n_intra),
        out_shape=(
            jax.ShapeDtypeStruct((owned, BLOCK), f32),
            jax.ShapeDtypeStruct((8, BLOCK), f32),
        ),
        in_specs=[pl.BlockSpec(memory_space=pl.ANY), vmem],
        out_specs=(vmem, vmem),
        scratch_shapes=[
            pltpu.VMEM((SLOTS, owned, columns), jnp.bfloat16),
            pltpu.VMEM((n_intra, n_hi, 2, 2, half, BLOCK), f32),
            pltpu.VMEM((n_z, n_hi, 2, 2, half, BLOCK), f32),
            pltpu.VMEM((2, 2, 2, half, BLOCK), f32),
            pltpu.VMEM((n_z, 2, 2, half, BLOCK), f32),
            pltpu.VMEM((n_z, 2, half, BLOCK), f32),
            pltpu.VMEM((n_z, 2, half, BLOCK), f32),
            pltpu.VMEM((2, 8, BLOCK), f32),
            pltpu.VMEM((group, 8, BLOCK), f32),
            pltpu.VMEM((n_z, 8, BLOCK), f32),
            dma((SLOTS,)),
            dma((n_z,)), dma((n_z,)),
            dma((2, 2)), dma((2, 2)),
            dma((2, n_z)), dma((2, n_z)),
            dma((2, n_z)), dma((2, n_z)),
            dma((n_z,)), dma((n_z,)),
            dma((group,)), dma((group,)),
            dma((n_z,)), dma((n_z,)),
        ],
        compiler_params=pltpu.CompilerParams(
            collective_id=0, has_side_effects=True, vmem_limit_bytes=60 * 1024 * 1024
        ),
    )(local, sign_table)
    shape = jax.ShapeDtypeStruct((owned, BLOCK), f32)
    return pl.pallas_call(
        functools.partial(adam_kernel, float(n_node * n_intra)),
        out_shape=(shape, shape, shape),
        in_specs=[vmem, vmem, vmem, smem, smem, vmem, vmem, vmem],
        out_specs=(vmem, vmem, vmem),
    )(summed, top, sign_table, loss_scale, step_count, weights, first_moment, second_moment)


def solution(mesh):
    own = P("intra", "node")
    return jax.shard_map(
        shards,
        mesh=mesh,
        in_specs=(P("node", "intra", None, None), P(), P(), P(), own, own, own),
        out_specs=(own, own, own),
        check_vma=False,
    )
```

```python
import functools
import math

import jax
import jax.numpy as jnp
from jax import lax
from jax.experimental import pallas as pl
from jax.experimental.pallas import tpu as pltpu
from jax.sharding import PartitionSpec as P

BLOCK = 128
SIGN_ROWS = 64
CORES = 2
SLOTS = 4
SUBS = 2
ROOT = 1.0 / math.sqrt(BLOCK)
MESH = pl.DeviceIdType.MESH


def hadamard_table():
    common = lax.broadcasted_iota(jnp.int32, (BLOCK, BLOCK), 0) & lax.broadcasted_iota(
        jnp.int32, (BLOCK, BLOCK), 1
    )
    parity = common
    for bit_index in range(1, BLOCK.bit_length() - 1):
        parity = parity ^ (common >> bit_index)
    return (1 - 2 * (parity & 1)).astype(jnp.float32).astype(jnp.bfloat16)


def reduce_kernel(
    n_node, n_intra, grad_ref, sign_ref, sum_ref, top_ref,
    stage, lev, pair, raw, first, second, third, peak, near, far,
    load_sem, pair_send, pair_recv, raw_send, raw_recv, first_send, first_recv,
    second_send, second_recv, third_send, third_recv, near_send, near_recv, far_send, far_recv,
):
    lo_count = 2
    n_z = n_intra // CORES
    owned = lev.shape[4] * 2
    half = owned // 2
    node, intra = lax.axis_index("node"), lax.axis_index("intra")
    z, core = intra // CORES, intra % CORES
    hi, lo = node // lo_count, node % lo_count
    group = n_node * CORES
    me = node * CORES + core

    def at(node_index, z_index, core_index):
        return (node_index, z_index * CORES + core_index)

    def send(src, dst, send_sem, recv_sem, device):
        return pltpu.make_async_remote_copy(
            src_ref=src, dst_ref=dst, send_sem=send_sem, recv_sem=recv_sem,
            device_id=device, device_id_type=MESH,
        )

    def piece(k):
        last = n_z - 1
        lower = jnp.where(k < last - z, last - k, k - (last - z))
        upper = jnp.where(k < z, k, last - (k - z))
        return jnp.where(z < n_z // 2, lower, upper)

    early = min(2, n_z)

    def block_at(q):
        other = (q >= early) & (q < early + n_z)
        k = jnp.where(q < early, q, jnp.where(other, q - early, q - n_z))
        return piece(k) * CORES + jnp.where(other, 1 - core, core)

    def load(q):
        slot = lax.rem(q, SLOTS)
        return pltpu.make_async_copy(
            grad_ref.at[pl.ds(block_at(q) * owned, owned)], stage.at[slot], load_sem.at[slot]
        )

    for q in range(min(SLOTS, n_intra)):
        load(q).start()

    barrier = pltpu.get_barrier_semaphore()
    for step in range(1, group):
        other = lax.rem(me + step, group)
        pl.semaphore_signal(
            barrier, inc=1, device_id=at(other // CORES, z, other % CORES), device_id_type=MESH
        )
    for step in range(1, n_z):
        pl.semaphore_signal(
            barrier, inc=1, device_id=at(node, lax.rem(z + step, n_z), core), device_id_type=MESH
        )

    table = hadamard_table()
    signs = sign_ref[...].astype(jnp.float32).astype(jnp.bfloat16)

    def rotate(q, most):
        load(q).wait()
        i = block_at(q)
        block = stage[lax.rem(q, SLOTS)]
        for j in range(n_node):
            cols = slice(j * BLOCK, (j + 1) * BLOCK)
            part = block[:, cols].reshape(owned // SIGN_ROWS, SIGN_ROWS, BLOCK)
            signed = (part * signs[:, cols][None]).reshape(owned, BLOCK)
            spun = jnp.dot(signed, table, preferred_element_type=jnp.float32) * ROOT
            for h in range(2):
                lev[i, j // lo_count, j % lo_count, h] = spun[h * half : (h + 1) * half]
            most = jnp.maximum(most, jnp.max(jnp.abs(spun).reshape(owned // 8, 8, BLOCK), axis=0))

        @pl.when(q + SLOTS < n_intra)
        def _():
            load(q + SLOTS).start()

        return most

    lo_peer = hi * lo_count + 1 - lo
    hi_peer = (1 - hi) * lo_count + lo

    def pair_copy(p):
        return send(
            lev.at[p * CORES + 1 - core], pair.at[p], pair_send.at[p], pair_recv.at[p],
            at(node, z, 1 - core),
        )

    def raw_copies(flip):
        target = core if flip == 0 else 1 - core
        i = piece(0) * CORES + target
        return [
            send(
                src, raw.at[flip, h], raw_send.at[flip, h], raw_recv.at[flip, h],
                at(peer, z, target),
            )
            for h, src, peer in (
                (0, lev.at[i, :, 1 - lo, 0], lo_peer),
                (1, lev.at[i, 1 - hi, :, 1], hi_peer),
            )
        ]

    part_rows = half // SUBS

    def rows_of(s):
        return pl.ds(s * part_rows, part_rows)

    def first_copies(p, s):
        i, r = p * CORES + core, rows_of(s)
        return [
            send(
                src, first.at[p, h, :, r], first_send.at[h, p * SUBS + s],
                first_recv.at[h, p * SUBS + s], at(peer, z, core),
            )
            for h, src, peer in (
                (0, lev.at[i, :, 1 - lo, 0, r], lo_peer),
                (1, lev.at[i, 1 - hi, :, 1, r], hi_peer),
            )
        ]

    def second_copies(p, s):
        i, r = p * CORES + core, rows_of(s)
        return [
            send(
                src, second.at[p, h, r], second_send.at[h, p * SUBS + s],
                second_recv.at[h, p * SUBS + s], at(peer, z, core),
            )
            for h, src, peer in (
                (0, lev.at[i, 1 - hi, lo, 0, r], hi_peer),
                (1, lev.at[i, hi, 1 - lo, 1, r], lo_peer),
            )
        ]

    def third_copy(p, slot, s):
        r = rows_of(s)
        return send(
            lev.at[p * CORES + core, hi, lo, :, r], third.at[slot, :, r],
            third_send.at[p * SUBS + s], third_recv.at[slot * SUBS + s], at(node, p, core),
        )

    def near_copy(target, slot):
        return send(
            peak.at[0], near.at[slot], near_send.at[target], near_recv.at[slot],
            at(target // CORES, z, target % CORES),
        )

    def far_copy(target, slot):
        return send(
            peak.at[1], far.at[slot], far_send.at[target], far_recv.at[slot],
            at(node, target, core),
        )

    most = lax.fori_loop(0, early, rotate, jnp.zeros((8, BLOCK), jnp.float32))
    pl.semaphore_wait(barrier, group - 1 + n_z - 1)
    for copy in raw_copies(0):
        copy.start()

    def rotate_and_send(q, most):
        most = rotate(q, most)
        pair_copy(piece(q - early)).start()
        return most

    most = lax.fori_loop(early, early + n_z, rotate_and_send, most)
    most = lax.fori_loop(early + n_z, n_intra, rotate, most)

    peak[0] = most
    for step in range(1, group):
        near_copy(lax.rem(me + step, group), me).start()
    for copy in raw_copies(1):
        copy.start()
    for step in range(1, group):
        other = lax.rem(me + step, group)
        near_copy(other, other).wait_recv()
        most = jnp.maximum(most, near[other])
    peak[1] = most
    for step in range(1, n_z):
        far_copy(lax.rem(z + step, n_z), z).start()
    for step in range(1, n_z):
        other = lax.rem(z + step, n_z)
        far_copy(other, other).wait_recv()
        most = jnp.maximum(most, far[other])
    top_value = jnp.max(jnp.max(most, axis=0, keepdims=True), axis=1, keepdims=True)
    top_ref[...] = jnp.broadcast_to(top_value, (8, BLOCK))
    level_scale = 127.0 / top_value

    def level(value):
        return jnp.floor(value * level_scale + 0.5)

    items = n_z * SUBS

    def last_exchange(p, s):
        i, r = p * CORES + core, rows_of(s)
        for copy in second_copies(p, s):
            copy.wait_recv()
        for h in range(2):
            lev[i, hi, lo, h, r] = lev[i, hi, lo, h, r] + second[p, h, r]

        @pl.when(p != z)
        def _():
            third_copy(p, z, s).start()

    def pipeline(t, carry):
        @pl.when(t == SUBS)
        def _():
            pair_copy(piece(0)).wait_recv()

        @pl.when(t < items)
        def _():
            p, s = piece(t // SUBS), t % SUBS
            i, r = p * CORES + core, rows_of(s)

            @pl.when(s == 0)
            def _():
                pair_copy(p).wait_recv()

            for j in range(n_node):
                for h in range(2):
                    spot = (j // lo_count, j % lo_count, h, r)
                    lev[(i,) + spot] = level(lev[(i,) + spot]) + level(pair[(p,) + spot])
            for copy in first_copies(p, s):
                copy.start()

        @pl.when(t == SUBS)
        def _():
            p = piece(0)
            i = p * CORES + core
            for flip in range(2):
                for copy in raw_copies(flip):
                    copy.wait_recv()

            def kept(h, j, spot):
                lev[(i,) + spot] = (
                    level(lev[(i,) + spot]) + level(pair[(p,) + spot])
                    + level(raw[0, h, j]) + level(raw[1, h, j])
                )

            for j in range(2):
                kept(0, j, (j, lo, 0))
                kept(1, j, (hi, j, 1))
            for s in range(SUBS):
                for copy in second_copies(p, s):
                    copy.start()

        @pl.when((t > SUBS) & (t <= items))
        def _():
            p, s = piece((t - 1) // SUBS), (t - 1) % SUBS
            i, r = p * CORES + core, rows_of(s)
            for copy in first_copies(p, s):
                copy.wait_recv()
            for j in range(2):
                lev[i, j, lo, 0, r] = lev[i, j, lo, 0, r] + first[p, 0, j, r]
                lev[i, hi, j, 1, r] = lev[i, hi, j, 1, r] + first[p, 1, j, r]
            for copy in second_copies(p, s):
                copy.start()

        @pl.when(t == SUBS + 1)
        def _():
            for s in range(SUBS):
                last_exchange(piece(0), s)

        @pl.when(t >= SUBS + 2)
        def _():
            last_exchange(piece((t - 2) // SUBS), (t - 2) % SUBS)

        return carry

    lax.fori_loop(SUBS, items + 2, pipeline, 0)

    total = lev[intra, hi, lo]
    for step in range(1, n_z):
        other = lax.rem(z + step, n_z)
        for s in range(SUBS):
            third_copy(other, other, s).wait_recv()
        total = total + third[other]
    for h in range(2):
        sum_ref[h * half : (h + 1) * half, :] = total[h]

    for step in range(1, group):
        near_copy(lax.rem(me + step, group), me).wait_send()
    for step in range(1, n_z):
        far_copy(lax.rem(z + step, n_z), z).wait_send()
    for flip in range(2):
        for copy in raw_copies(flip):
            copy.wait_send()

    def finish(k, carry):
        p = piece(k)
        pair_copy(p).wait_send()
        for s in range(SUBS):
            for copy in second_copies(p, s):
                copy.wait_send()

        @pl.when(k > 0)
        def _():
            for s in range(SUBS):
                for copy in first_copies(p, s):
                    copy.wait_send()

        @pl.when(p != z)
        def _():
            for s in range(SUBS):
                third_copy(p, z, s).wait_send()

        return carry

    lax.fori_loop(0, n_z, finish, 0)


def adam_kernel(
    replicas, sum_ref, top_ref, sign_ref, scale_ref, step_ref,
    weight_ref, first_ref, second_ref, new_weight_ref, new_first_ref, new_second_ref,
):
    owned = sum_ref.shape[0]
    table = hadamard_table()
    column = pl.multiple_of(lax.axis_index("node") * BLOCK, BLOCK)
    summed = sum_ref[...]
    high = jnp.floor(summed * (1.0 / 64.0))
    low = summed - high * 64.0
    back = jnp.dot(high.astype(jnp.bfloat16), table, preferred_element_type=jnp.float32) * 64.0
    back = back + jnp.dot(low.astype(jnp.bfloat16), table, preferred_element_type=jnp.float32)
    ones = jnp.ones((1, BLOCK), jnp.float32)
    factor = top_ref[0:1, :] / (ones * (127.0 * replicas * scale_ref[0]))
    signs = sign_ref[:, pl.ds(column, BLOCK)].astype(jnp.float32) * (factor * ROOT)
    grad = (back.reshape(owned // SIGN_ROWS, SIGN_ROWS, BLOCK) * signs[None]).reshape(owned, BLOCK)
    steps = ones * step_ref[0].astype(jnp.float32)
    first_unbias = 1.0 / (1.0 - jnp.exp(steps * math.log(0.9)))
    second_unbias = 1.0 / (1.0 - jnp.exp(steps * math.log(0.95)))
    new_first = 0.9 * first_ref[...] + 0.1 * grad
    new_second = 0.95 * second_ref[...] + 0.05 * grad * grad
    new_first_ref[...] = new_first
    new_second_ref[...] = new_second
    weights = weight_ref[...]
    update = (new_first * first_unbias) / (jnp.sqrt(new_second * second_unbias) + 1e-08)
    new_weight_ref[...] = weights - 0.2 * (update + 0.1 * weights)


def shards(gradients, sign_table, loss_scale, step_count, weights, first_moment, second_moment):
    n_node, n_intra = lax.axis_size("node"), lax.axis_size("intra")
    n_z = n_intra // CORES
    local = gradients.reshape(gradients.shape[2:])
    rows, columns = local.shape
    owned = weights.shape[0]
    half = owned // 2
    n_hi = n_node // 2
    vmem = pl.BlockSpec(memory_space=pltpu.VMEM)
    smem = pl.BlockSpec(memory_space=pltpu.SMEM)
    dma = pltpu.SemaphoreType.DMA
    group = n_node * CORES
    f32 = jnp.float32
    summed, top = pl.pallas_call(
        functools.partial(reduce_kernel, n_node, n_intra),
        out_shape=(
            jax.ShapeDtypeStruct((owned, BLOCK), f32),
            jax.ShapeDtypeStruct((8, BLOCK), f32),
        ),
        in_specs=[pl.BlockSpec(memory_space=pl.ANY), vmem],
        out_specs=(vmem, vmem),
        scratch_shapes=[
            pltpu.VMEM((SLOTS, owned, columns), jnp.bfloat16),
            pltpu.VMEM((n_intra, n_hi, 2, 2, half, BLOCK), f32),
            pltpu.VMEM((n_z, n_hi, 2, 2, half, BLOCK), f32),
            pltpu.VMEM((2, 2, 2, half, BLOCK), f32),
            pltpu.VMEM((n_z, 2, 2, half, BLOCK), f32),
            pltpu.VMEM((n_z, 2, half, BLOCK), f32),
            pltpu.VMEM((n_z, 2, half, BLOCK), f32),
            pltpu.VMEM((2, 8, BLOCK), f32),
            pltpu.VMEM((group, 8, BLOCK), f32),
            pltpu.VMEM((n_z, 8, BLOCK), f32),
            dma((SLOTS,)),
            dma((n_z,)), dma((n_z,)),
            dma((2, 2)), dma((2, 2)),
            dma((2, n_z * SUBS)), dma((2, n_z * SUBS)),
            dma((2, n_z * SUBS)), dma((2, n_z * SUBS)),
            dma((n_z * SUBS,)), dma((n_z * SUBS,)),
            dma((group,)), dma((group,)),
            dma((n_z,)), dma((n_z,)),
        ],
        compiler_params=pltpu.CompilerParams(
            collective_id=0, has_side_effects=True, vmem_limit_bytes=60 * 1024 * 1024
        ),
    )(local, sign_table)
    shape = jax.ShapeDtypeStruct((owned, BLOCK), f32)
    return pl.pallas_call(
        functools.partial(adam_kernel, float(n_node * n_intra)),
        out_shape=(shape, shape, shape),
        in_specs=[vmem, vmem, vmem, smem, smem, vmem, vmem, vmem],
        out_specs=(vmem, vmem, vmem),
    )(summed, top, sign_table, loss_scale, step_count, weights, first_moment, second_moment)


def solution(mesh):
    own = P("intra", "node")
    return jax.shard_map(
        shards,
        mesh=mesh,
        in_specs=(P("node", "intra", None, None), P(), P(), P(), own, own, own),
        out_specs=(own, own, own),
        check_vma=False,
    )
```
